32 devices in a mesh: row: 4 (over y, x), col: 4 (over z), head: 2 (over core).
Axes of the slice: x: 2, y: 2, z: 4, core: 2. Of those that a mesh axis runs over, the one named last changes fastest.
Arguments:
- queries: bfloat16 [256, 64, 256], P('row', 'col'), may hold values from -1000 to 1000
- level_zero: bfloat16 [256, 64, 256], P('row', 'col', 'head'), may hold values from -6 to 6
- level_one: bfloat16 [128, 32, 256], P('row', 'col', 'head'), may hold values from -6 to 6
- level_two: bfloat16 [64, 16, 256], P('row', 'col', 'head'), may hold values from -6 to 6
- level_three: bfloat16 [32, 8, 256], P('row', 'col', 'head'), may hold values from -6 to 6
- tile_lists: int32 [16, 4, 4, 8], P('row', 'col'), may hold values from 0 to 63, as said below
- samples: int32 [256, 64, 128], P('row', 'col', 'head'), may hold values from 0 to 133168895, as said below
- logit_weight: bfloat16 [256, 128], P(None, 'head'), may hold values from -1 to 1
- logit_bias: float32 [128], P('head'), may hold values from -3 to 3
- output_weight: bfloat16 [256, 256], replicated, may hold values from -0.375 to 0.375
- output_bias: float32 [256], replicated, may hold values from -3 to 3
- norm_gain: float32 [256], P('head'), may hold values from 0.5 to 1.5
- norm_shift: float32 [256], P('head'), may hold values from -3 to 3
Outputs:
- updated_queries: bfloat16 [256, 64, 256], P('row', 'col', 'head')
The draws below stay inside these ranges and needn't reach their ends.
Inputs may be any that keep to these rules, and one draw needn't show every extreme that they name: `tile_lists`: entries are tile numbers r * 4 + c. Over all lists of the query blocks that one device holds, at one level, at most 2 entries name tiles that one device holds; at each level some device is named exactly 2 times by the lists of every device. A tile may be listed more than once. `samples`: slot is below 8; at level l, pos_row and pos_col are below (16 / 2^l - 1) * 256.
All inputs are finite; a program needn't handle non-finite values.
Results may differ from the reference program's by a relative error of at most 0.004.
Values may be sent and summed in bfloat16 or wider, within the bound.
A program may use at most 128 MiB of HBM per device.

```python
import math
import jax
import jax.numpy as jnp
from jax import lax

D = 256
HEADS = 8
LEVELS = 4
POINTS = 4
TILE = 16
K = 8
TR = 4
TC = 1
ROWS = 256
COLS = 64
N_ROW = 4
N_COL = 4


def attend_columns(key):
    raw_draw = jax.random.normal(jax.random.fold_in(key, 701), (D, HEADS * LEVELS * POINTS), jnp.float32)
    return (jnp.clip(raw_draw, -5.0, 5.0) / math.sqrt(D)).astype(jnp.bfloat16)


def draw_logit_weight(key, part):
    return attend_columns(key)


def draw_queries(key, part):
    height = TR * TILE * N_ROW
    width_all = TC * TILE * N_COL
    base_draw = jax.random.normal(jax.random.fold_in(key, 1), (height, width_all, D), jnp.float32)
    base_draw = jnp.clip(base_draw, -6.0, 6.0)
    return base_draw.astype(jnp.bfloat16)


def draw_samples(key, part):
    height = TR * TILE * N_ROW
    width_all = TC * TILE * N_COL
    lane_count = HEADS * LEVELS * POINTS
    lane_level = jnp.arange(lane_count, dtype=jnp.int32) // POINTS % LEVELS
    pos_limit = (TILE // jnp.left_shift(jnp.int32(1), lane_level) - 1) * 256
    full_shape = (height, width_all, lane_count)
    slot_draw = jax.random.randint(jax.random.fold_in(key, 21), full_shape, 0, K)
    row_draw = jax.random.randint(jax.random.fold_in(key, 22), full_shape, 0, jnp.broadcast_to(pos_limit, full_shape))
    col_draw = jax.random.randint(jax.random.fold_in(key, 23), full_shape, 0, jnp.broadcast_to(pos_limit, full_shape))
    return (slot_draw * 16777216 + row_draw * 4096 + col_draw).astype(jnp.int32)


def draw_tile_lists(key, part):
    peer_count = N_ROW * N_COL
    local_tiles = TR * TC
    requests = local_tiles * K
    capacity = max(2, (requests + peer_count - 1) // peer_count)
    slot_count = peer_count * capacity
    hot_owner = jax.random.randint(jax.random.fold_in(key, 31), (LEVELS,), 0, peer_count)

    def one_list(device_num, level_num):
        sub_key = jax.random.fold_in(jax.random.fold_in(key, 32), device_num * LEVELS + level_num)
        scores = jax.random.permutation(jax.random.fold_in(sub_key, 1), slot_count).astype(jnp.int32)
        forced = jnp.arange(slot_count, dtype=jnp.int32) // capacity == hot_owner[level_num]
        scores = jnp.where(forced, -1, scores)
        ranking = jnp.argsort(scores, stable=True)
        chosen = ranking[:requests]
        chosen = chosen[jax.random.permutation(jax.random.fold_in(sub_key, 2), requests)]
        owner_dev = chosen.astype(jnp.int32) // capacity
        local_index = jax.random.randint(jax.random.fold_in(sub_key, 3), (requests,), 0, local_tiles)
        tile_row = owner_dev // N_COL * TR + local_index // TC
        tile_col = owner_dev % N_COL * TC + local_index % TC
        return (tile_row * (TC * N_COL) + tile_col).astype(jnp.int32)
    device_grid = jnp.arange(peer_count, dtype=jnp.int32)
    level_grid = jnp.arange(LEVELS, dtype=jnp.int32)
    tile_ids = jax.vmap(lambda device_num: jax.vmap(lambda level_num: one_list(device_num, level_num))(level_grid))(device_grid)
    tile_ids = tile_ids.reshape(N_ROW, N_COL, LEVELS, TR, TC, K)
    return tile_ids.transpose(0, 3, 1, 4, 2, 5).reshape(TR * N_ROW, TC * N_COL, LEVELS, K)


def levels(rng, dims, split, least, largest):
    gain = 1.0
    for position, shards_of in split:
        heights = jax.random.uniform(jax.random.fold_in(jax.random.fold_in(rng, 6), position), (shards_of,), jnp.float32, least / len(split), largest / len(split))
        gain = gain * jnp.repeat(jnp.exp(heights), dims[position] // shards_of).reshape((-1,) + (1,) * (len(dims) - 1 - position))
    return gain


def scatter_about(key, shape, deviation, most, cuts=(), kind=jnp.bfloat16):
    values = jax.random.normal(key, shape, jnp.float32) * deviation
    if len(cuts) > 0:
        values = levels(key, shape, cuts, -0.22, 0.18) * values
    return jnp.clip(values, min=-most, max=most).astype(kind)


def setup_inputs(seed: int = 0) -> dict:
    key_list = jax.random.split(jax.random.key(seed), 14)
    queries = draw_queries(jax.random.fold_in(key_list[13], 71), 0)
    level_zero = scatter_about(key_list[1], (ROWS, COLS, D), 1.0, 6.0, ((0, 4), (1, 4), (2, 2)))
    level_one = scatter_about(key_list[2], (ROWS // 2, COLS // 2, D), 1.0, 6.0, ((0, 4), (1, 4), (2, 2)))
    level_two = scatter_about(key_list[3], (ROWS // 4, COLS // 4, D), 1.0, 6.0, ((0, 4), (1, 4), (2, 2)))
    level_three = scatter_about(key_list[4], (ROWS // 8, COLS // 8, D), 1.0, 6.0, ((0, 4), (1, 4), (2, 2)))
    tile_lists = draw_tile_lists(jax.random.fold_in(key_list[13], 71), 0)
    samples = draw_samples(jax.random.fold_in(key_list[13], 71), 0)
    logit_weight = draw_logit_weight(jax.random.fold_in(key_list[13], 71), 0)
    logit_bias = scatter_about(key_list[8], (HEADS * LEVELS * POINTS,), 0.5, 3.0, ((0, 2),), jnp.float32)
    output_weight = scatter_about(key_list[9], (D, D), D ** -0.5, 0.375)
    output_bias = scatter_about(key_list[10], (D,), 0.5, 3.0, (), jnp.float32)
    norm_gain = jnp.clip(1.0 + 0.1 * jax.random.normal(key_list[11], (D,), jnp.float32), 0.5, 1.5)
    norm_shift = scatter_about(key_list[12], (D,), 0.5, 3.0, ((0, 2),), jnp.float32)
    return dict(queries=queries, level_zero=level_zero, level_one=level_one, level_two=level_two, level_three=level_three, tile_lists=tile_lists, samples=samples, logit_weight=logit_weight, logit_bias=logit_bias, output_weight=output_weight, output_bias=output_bias, norm_gain=norm_gain, norm_shift=norm_shift)


def to_blocks(source, grid_rows, grid_cols, tile_side):
    channels = source.shape[2]
    shaped = source.reshape(grid_rows, tile_side, grid_cols, tile_side, channels)
    return shaped.transpose(0, 2, 1, 3, 4).reshape(grid_rows * grid_cols, tile_side * tile_side, channels)

def reference(queries, level_zero, level_one, level_two, level_three, tile_lists, samples, logit_weight, logit_bias, output_weight, output_bias, norm_gain, norm_shift):
    grid_rows = tile_lists.shape[0]
    grid_cols = tile_lists.shape[1]
    head_dim = D // HEADS
    pixels = TILE * TILE
    hits = POINTS * 4
    tile_sets = []
    for level_num, level_array in enumerate((level_zero, level_one, level_two, level_three)):
        tile_side = TILE // 2 ** level_num
        blocks_here = to_blocks(level_array, grid_rows, grid_cols, tile_side)
        tile_sets.append(blocks_here.reshape(grid_rows * grid_cols, tile_side * tile_side, HEADS, head_dim))
    query_blocks = to_blocks(queries, grid_rows, grid_cols, TILE)
    sample_blocks = to_blocks(samples, grid_rows, grid_cols, TILE)
    list_blocks = tile_lists.reshape(grid_rows * grid_cols, LEVELS, K)
    earlier = jnp.arange(hits, dtype=jnp.int32)[None, :] < jnp.arange(hits, dtype=jnp.int32)[:, None]

    def one_block(operands):
        query_blk, sample_blk, list_blk = operands
        logits = jnp.dot(query_blk, logit_weight, preferred_element_type=jnp.float32) + logit_bias
        attend = jax.nn.softmax(logits.reshape(pixels, HEADS, LEVELS * POINTS), axis=-1)
        attend = attend.reshape(pixels, HEADS, LEVELS, POINTS)
        packed = sample_blk.reshape(pixels, HEADS, LEVELS, POINTS)
        slot_index = packed // 16777216
        pos_row = packed // 4096 % 4096
        pos_col = packed % 4096
        frac_row = (pos_row % 256).astype(jnp.float32) / 256.0
        frac_col = (pos_col % 256).astype(jnp.float32) / 256.0
        running = jnp.zeros((pixels, HEADS, head_dim), jnp.float32)
        for level_num in range(LEVELS):
            tile_side = TILE // 2 ** level_num
            chosen = tile_sets[level_num][list_blk[level_num]]
            flat_values = chosen.reshape(K * tile_side * tile_side, HEADS, head_dim).transpose(1, 0, 2)
            base_index = slot_index[:, :, level_num] * tile_side * tile_side + pos_row[:, :, level_num] // 256 * tile_side + pos_col[:, :, level_num] // 256
            lvl_row = frac_row[:, :, level_num]
            lvl_col = frac_col[:, :, level_num]
            attend_lvl = attend[:, :, level_num]
            targets = jnp.stack([base_index, base_index + 1, base_index + tile_side, base_index + tile_side + 1], axis=3).reshape(pixels, HEADS, hits)
            corner_weights = jnp.stack([attend_lvl * (1.0 - lvl_row) * (1.0 - lvl_col), attend_lvl * (1.0 - lvl_row) * lvl_col, attend_lvl * lvl_row * (1.0 - lvl_col), attend_lvl * lvl_row * lvl_col], axis=3).reshape(pixels, HEADS, hits)
            same_pixel = targets[:, :, :, None] == targets[:, :, None, :]
            combined = lax.optimization_barrier(jnp.sum(jnp.where(same_pixel, corner_weights[:, :, None, :], 0.0), axis=3))
            repeated = jnp.any(same_pixel & earlier, axis=3)
            rounded = lax.optimization_barrier(combined.astype(jnp.bfloat16)).astype(jnp.float32)
            pixel_weight = jnp.where(repeated, 0.0, rounded)
            lookup = targets.transpose(1, 0, 2).reshape(HEADS, pixels * hits)
            picked = jnp.take_along_axis(flat_values, lookup[:, :, None], axis=1).astype(jnp.float32)
            picked = picked.reshape(HEADS, pixels, hits, head_dim)
            running = running + jnp.einsum('qhn,hqnd->qhd', pixel_weight, picked, precision=lax.Precision.HIGHEST)
        attn_out = running.reshape(pixels, D).astype(jnp.bfloat16)
        pre_norm = query_blk.astype(jnp.float32) + jnp.dot(attn_out, output_weight, preferred_element_type=jnp.float32) + output_bias
        row_mean = lax.optimization_barrier(jnp.mean(pre_norm, axis=1, keepdims=True))
        centered = pre_norm - row_mean
        variance = lax.optimization_barrier(jnp.mean(centered * centered, axis=1, keepdims=True))
        return (centered * lax.rsqrt(variance + 1e-05) * norm_gain + norm_shift).astype(jnp.bfloat16)
    updated = lax.map(one_block, (query_blocks, sample_blocks, list_blocks))
    updated = updated.reshape(grid_rows, grid_cols, TILE, TILE, D).transpose(0, 2, 1, 3, 4)
    return updated.reshape(grid_rows * TILE, grid_cols * TILE, D)
```

```python
import functools

import jax
import jax.numpy as jnp
from jax import lax
from jax.experimental import pallas as pl
from jax.experimental.pallas import tpu as pltpu
from jax.sharding import PartitionSpec as P

LEVELS = 4
POINTS = 4
PACK = 16


def to_blocks(source, tile_rows, tile_cols, tile_side):
    channels = source.shape[2]
    shaped = source.reshape(tile_rows, tile_side, tile_cols, tile_side, channels)
    return shaped.transpose(0, 2, 1, 3, 4).reshape(
        tile_rows * tile_cols, tile_side * tile_side, channels
    )


def weight_kernel(sides, spans, per_block, head_count, query_ref, lw_ref, lb_ref, samples_ref,
                  out_ref, row_s, col_s, w0_s, w1_s, g0_s, g1_s, slot_s, mask_s):
    queries_here = query_ref.shape[1]
    hits = LEVELS * POINTS
    logits = lax.dot_general(
        lw_ref[...], query_ref[0], (((1,), (1,)), ((), ())), preferred_element_type=jnp.float32
    ) + lb_ref[...]
    logits = logits.reshape(head_count, hits, queries_here)
    shifted = jnp.exp(logits - jnp.max(logits, axis=1, keepdims=True))
    attend = shifted / jnp.sum(shifted, axis=1, keepdims=True)
    attend = attend.reshape(head_count * hits, queries_here)
    packed = samples_ref[0]
    pos_row = (packed >> 12) & 4095
    pos_col = packed & 4095
    frac_row = (pos_row & 255).astype(jnp.float32) * (1.0 / 256.0)
    frac_col = (pos_col & 255).astype(jnp.float32) * (1.0 / 256.0)
    slot_s[...] = packed >> 24
    row_s[...] = pos_row >> 8
    col_s[...] = pos_col >> 8
    w0_s[...] = attend * (1.0 - frac_row)
    w1_s[...] = attend * frac_row
    g0_s[...] = 1.0 - frac_col
    g1_s[...] = frac_col
    lane_row = lax.broadcasted_iota(jnp.int32, (PACK, queries_here), 0)
    slot_row = lax.broadcasted_iota(jnp.int32, (per_block, queries_here), 0)

    def hat(index, start, low, high):
        return jnp.where(index == start, low, jnp.where(index == start + 1, high, 0.0))

    def one_head(h, carry):
        level_off = 0
        for level_num in range(LEVELS):
            side = sides[level_num]
            span = spans[level_num]
            rows = [pl.ds(h * hits + level_num * POINTS + p, 1) for p in range(POINTS)]
            for p in range(POINTS):
                mask_s[p * per_block:(p + 1) * per_block, :] = jnp.where(
                    slot_row == slot_s[rows[p], :], 1.0, 0.0
                )
            cols = [
                hat(lane_row % side, col_s[rows[p], :], g0_s[rows[p], :], g1_s[rows[p], :])
                for p in range(POINTS)
            ]
            rows_per_chunk = PACK // side

            def chunk(step, carry, rows=rows, cols=cols, side=side, span=span,
                      level_off=level_off, rows_per_chunk=rows_per_chunk):
                parts = []
                for p in range(POINTS):
                    index = step * rows_per_chunk
                    if rows_per_chunk > 1:
                        index = index + lane_row // side
                        across = hat(index, row_s[rows[p], :], w0_s[rows[p], :], w1_s[rows[p], :])
                    else:
                        start = row_s[rows[p], :]
                        across = jnp.where(
                            start == index,
                            w0_s[rows[p], :],
                            jnp.where(start == index - 1, w1_s[rows[p], :], 0.0),
                        )
                    parts.append(cols[p] * across)
                for k in range(per_block):
                    total = parts[0] * mask_s[k:k + 1, :]
                    for p in range(1, POINTS):
                        total = total + parts[p] * mask_s[p * per_block + k:p * per_block + k + 1, :]
                    where = pl.multiple_of(level_off + k * span + step * PACK, PACK)
                    out_ref[0, h, pl.ds(where, PACK), :] = total.astype(jnp.bfloat16)
                return carry

            chunks = span // PACK
            if chunks == 1:
                chunk(0, 0)
            else:
                lax.fori_loop(0, chunks, chunk, 0)
            level_off += span * per_block
        return carry

    lax.fori_loop(0, head_count, one_head, 0)


def pick_kernel(spans, peer_count, capacity, ids_ref, l0, l1, l2, l3, out_ref, sem):
    tiles = (l0, l1, l2, l3)

    def one(slot, carry):
        peer = slot // capacity
        place = slot % capacity
        off = 0
        for level_num in range(LEVELS):
            span = spans[level_num]
            index = jnp.maximum(ids_ref[peer, level_num * capacity + place], 0)
            pltpu.make_async_copy(
                tiles[level_num].at[pl.ds(pl.multiple_of(index * span, PACK), span), :],
                out_ref.at[slot, pl.ds(off, span), :],
                sem,
            ).start()
            off += span
        return carry

    lax.fori_loop(0, peer_count * capacity, one, 0)
    pltpu.make_async_copy(out_ref, out_ref, sem).wait()


def mix_kernel(spans, per_block, head_count, head_dim, pos_ref, fetched_ref, weight_ref, out_ref,
               values, values_t, mixed, sem):
    block = pl.program_id(0)
    h = pl.program_id(1)
    blocks = pl.num_programs(0)

    def fetch(which):
        off = 0
        src = 0
        for level_num in range(LEVELS):
            span = spans[level_num]
            for k in range(per_block):
                pltpu.make_async_copy(
                    fetched_ref.at[pos_ref[level_num, which * per_block + k], pl.ds(src, span), :],
                    values.at[which % 2, pl.ds(off, span), :],
                    sem.at[which % 2],
                ).start()
                off += span
            src += span

    @pl.when((h == 0) & (block == 0))
    def _():
        fetch(block)

    @pl.when(h == 0)
    def _():
        side = block % 2
        pltpu.make_async_copy(values.at[side], values.at[side], sem.at[side]).wait()
        values_t[...] = values[side].T.reshape(values_t.shape)

        @pl.when(block + 1 < blocks)
        def _():
            fetch(block + 1)

    mixed[h] = jnp.dot(values_t[h], weight_ref[0, 0], preferred_element_type=jnp.float32)

    @pl.when(h == head_count - 1)
    def _():
        whole = mixed[...].reshape(head_count * head_dim, mixed.shape[2])
        out_ref[...] = whole.T.astype(jnp.bfloat16)


def on_device(
    queries,
    level_zero,
    level_one,
    level_two,
    level_three,
    tile_lists,
    samples,
    logit_weight,
    logit_bias,
    output_weight,
    output_bias,
    norm_gain,
    norm_shift,
):
    level_blocks = (level_zero, level_one, level_two, level_three)
    row_count = lax.axis_size("row")
    col_count = lax.axis_size("col")
    peer_count = row_count * col_count
    tile_rows, tile_cols, level_count, per_block = tile_lists.shape
    local_tiles = tile_rows * tile_cols
    requests = local_tiles * per_block
    capacity = max(2, (requests + peer_count - 1) // peer_count)
    slots = peer_count * capacity
    grid_cols = tile_cols * col_count
    channels = level_zero.shape[2]
    width_all = queries.shape[2]
    head_count = samples.shape[2] // (LEVELS * POINTS)
    head_dim = channels // head_count
    tile_side = level_zero.shape[0] // tile_rows
    pixels = tile_side * tile_side
    sides = [level_blocks[level_num].shape[0] // tile_rows for level_num in range(level_count)]
    spans = [max(PACK, side * side) for side in sides]
    tile_span = sum(spans)
    depth = per_block * tile_span

    wanted = tile_lists.transpose(2, 0, 1, 3).reshape(level_count, requests)
    grid_row = wanted // grid_cols
    grid_col = wanted % grid_cols
    owner_dev = grid_row // tile_rows * col_count + grid_col // tile_cols
    local_index = grid_row % tile_rows * tile_cols + grid_col % tile_cols
    order = jnp.arange(requests, dtype=jnp.int32)
    earlier = (owner_dev[:, :, None] == owner_dev[:, None, :]) & (order[None, :] < order[:, None])
    positions = owner_dev * capacity + jnp.sum(earlier.astype(jnp.int32), axis=2)
    slot_order = jnp.arange(slots, dtype=jnp.int32)
    named = positions[:, None, :] == slot_order[None, :, None]
    slot_table = jnp.max(jnp.where(named, local_index[:, None, :], -1), axis=2)
    send_ids = slot_table.reshape(level_count, peer_count, capacity).transpose(1, 0, 2)
    asked = lax.all_to_all(
        send_ids.reshape(peer_count, level_count * capacity),
        ("row", "col"), split_axis=0, concat_axis=0, tiled=True,
    )

    tiles_local = []
    for level_num in range(level_count):
        tiles = to_blocks(level_blocks[level_num], tile_rows, tile_cols, sides[level_num])
        short = spans[level_num] - tiles.shape[1]
        if short > 0:
            tiles = jnp.pad(tiles, ((0, 0), (0, short), (0, 0)))
        tiles_local.append(tiles.reshape(local_tiles * spans[level_num], channels))
    vmem = pl.BlockSpec(memory_space=pltpu.VMEM)
    replies = pl.pallas_call(
        functools.partial(pick_kernel, spans, peer_count, capacity),
        out_shape=jax.ShapeDtypeStruct((slots, tile_span, channels), jnp.bfloat16),
        in_specs=[pl.BlockSpec(memory_space=pltpu.SMEM)] + [vmem] * 4,
        out_specs=pl.BlockSpec(memory_space=pl.ANY),
        scratch_shapes=[pltpu.SemaphoreType.DMA],
        name="pick",
    )(asked, *tiles_local)
    fetched = lax.all_to_all(
        replies.reshape(peer_count, capacity * tile_span, channels),
        ("row", "col"), split_axis=0, concat_axis=0, tiled=True,
    ).reshape(slots, tile_span, channels)

    queries_blocked = to_blocks(queries, tile_rows, tile_cols, tile_side)
    samples_t = to_blocks(samples, tile_rows, tile_cols, tile_side).transpose(0, 2, 1)
    lanes = head_count * LEVELS * POINTS
    lane_f32 = pltpu.VMEM((lanes, pixels), jnp.float32)
    lane_i32 = pltpu.VMEM((lanes, pixels), jnp.int32)
    weights = pl.pallas_call(
        functools.partial(weight_kernel, sides, spans, per_block, head_count),
        grid=(local_tiles,),
        out_shape=jax.ShapeDtypeStruct((local_tiles, head_count, depth, pixels), jnp.bfloat16),
        in_specs=[
            pl.BlockSpec((1, pixels, width_all), lambda b: (b, 0, 0)),
            pl.BlockSpec((lanes, width_all), lambda b: (0, 0)),
            pl.BlockSpec((lanes, 1), lambda b: (0, 0)),
            pl.BlockSpec((1, lanes, pixels), lambda b: (b, 0, 0)),
        ],
        out_specs=pl.BlockSpec((1, head_count, depth, pixels), lambda b: (b, 0, 0, 0)),
        scratch_shapes=[lane_i32, lane_i32, lane_f32, lane_f32, lane_f32, lane_f32, lane_i32,
                        pltpu.VMEM((POINTS * per_block, pixels), jnp.float32)],
        compiler_params=pltpu.CompilerParams(vmem_limit_bytes=40 * 1024 * 1024),
        cost_estimate=pl.CostEstimate(
            flops=8 * local_tiles * head_count * depth * pixels * POINTS,
            bytes_accessed=2 * local_tiles * head_count * depth * pixels, transcendentals=0,
        ),
        name="weights",
    )(queries_blocked, logit_weight.T, logit_bias[:, None], samples_t)

    attn_out = pl.pallas_call(
        functools.partial(mix_kernel, spans, per_block, head_count, head_dim),
        grid_spec=pltpu.PrefetchScalarGridSpec(
            num_scalar_prefetch=1,
            grid=(local_tiles, head_count),
            in_specs=[
                pl.BlockSpec(memory_space=pl.ANY),
                pl.BlockSpec((1, 1, depth, pixels), lambda b, h, pos: (b, h, 0, 0)),
            ],
            out_specs=pl.BlockSpec((pixels, channels), lambda b, h, pos: (b, 0)),
            scratch_shapes=[
                pltpu.VMEM((2, depth, channels), jnp.bfloat16),
                pltpu.VMEM((head_count, head_dim, depth), jnp.bfloat16),
                pltpu.VMEM((head_count, head_dim, pixels), jnp.float32),
                pltpu.SemaphoreType.DMA((2,)),
            ],
        ),
        out_shape=jax.ShapeDtypeStruct((local_tiles * pixels, channels), jnp.bfloat16),
        compiler_params=pltpu.CompilerParams(
            dimension_semantics=("arbitrary", "arbitrary"), vmem_limit_bytes=24 * 1024 * 1024
        ),
        cost_estimate=pl.CostEstimate(
            flops=2 * local_tiles * depth * pixels * channels,
            bytes_accessed=2 * local_tiles * head_count * depth * pixels, transcendentals=0,
        ),
        name="mix",
    )(positions, fetched, weights)

    head_index = lax.axis_index("head")
    full_attn = lax.all_gather(attn_out, "head", axis=1, tiled=True)
    pre_norm = (
        queries_blocked.reshape(local_tiles * pixels, width_all).astype(jnp.float32)
        + jnp.dot(full_attn, output_weight, preferred_element_type=jnp.float32)
        + output_bias
    )
    row_mean = jnp.mean(pre_norm, axis=1, keepdims=True)
    centered = pre_norm - row_mean
    variance = jnp.mean(centered * centered, axis=1, keepdims=True)
    own_part = lax.dynamic_slice_in_dim(centered, head_index * channels, channels, 1)
    normalized = own_part * lax.rsqrt(variance + 1e-05)
    updated = (normalized * norm_gain + norm_shift).astype(jnp.bfloat16)
    updated = updated.reshape(tile_rows, tile_cols, tile_side, tile_side, channels).transpose(
        0, 2, 1, 3, 4
    )
    return updated.reshape(tile_rows * tile_side, tile_cols * tile_side, channels)


def solution(mesh):
    in_specs = (
        P("row", "col", None),
        P("row", "col", "head"),
        P("row", "col", "head"),
        P("row", "col", "head"),
        P("row", "col", "head"),
        P("row", "col", None, None),
        P("row", "col", "head"),
        P(None, "head"),
        P("head"),
        P(),
        P(),
        P("head"),
        P("head"),
    )
    out_specs = P("row", "col", "head")
    return jax.shard_map(
        on_device, mesh=mesh, in_specs=in_specs, out_specs=out_specs, check_vma=False
    )
```

```python
import functools

import jax
import jax.numpy as jnp
from jax import lax
from jax.experimental import pallas as pl
from jax.experimental.pallas import tpu as pltpu
from jax.sharding import PartitionSpec as P

LEVELS = 4
POINTS = 4
PACK = 16
MESH = pl.DeviceIdType.MESH


def to_blocks(source, tile_rows, tile_cols, tile_side):
    channels = source.shape[2]
    shaped = source.reshape(tile_rows, tile_side, tile_cols, tile_side, channels)
    return shaped.transpose(0, 2, 1, 3, 4).reshape(
        tile_rows * tile_cols, tile_side * tile_side, channels
    )


def hat(index, start, low, high):
    return jnp.where(index == start, low, jnp.where(index == start + 1, high, 0.0))


def prepare(head_count, b, query_ref, lw_ref, lb_ref, samples_ref, point_s, corner_s):
    queries_here = query_ref.shape[1]
    hits = LEVELS * POINTS
    logits = lax.dot_general(
        lw_ref[...], query_ref[b], (((1,), (1,)), ((), ())), preferred_element_type=jnp.float32
    ) + lb_ref[...]
    logits = logits.reshape(head_count, hits, queries_here)
    shifted = jnp.exp(logits - jnp.max(logits, axis=1, keepdims=True))
    attend = shifted / jnp.sum(shifted, axis=1, keepdims=True)
    attend = attend.reshape(head_count * hits, queries_here)
    packed = samples_ref[b]
    pos_row = (packed >> 12) & 4095
    pos_col = packed & 4095
    frac_row = (pos_row & 255).astype(jnp.float32) * (1.0 / 256.0)
    frac_col = (pos_col & 255).astype(jnp.float32) * (1.0 / 256.0)
    point_s[b, 0] = packed >> 24
    point_s[b, 1] = pos_row >> 8
    point_s[b, 2] = pos_col >> 8
    corner_s[b, 0] = attend * (1.0 - frac_row)
    corner_s[b, 1] = attend * frac_row
    corner_s[b, 2] = 1.0 - frac_col
    corner_s[b, 3] = frac_col


def weigh(sides, spans, per_block, b, h, slab, point_s, corner_s, mask_s, weight_s):
    hits = LEVELS * POINTS
    queries_here = weight_s.shape[2]
    lane_row = lax.broadcasted_iota(jnp.int32, (PACK, queries_here), 0)
    slot_row = lax.broadcasted_iota(jnp.int32, (per_block, queries_here), 0)
    level_off = 0
    for level_num in range(LEVELS):
        side = sides[level_num]
        span = spans[level_num]
        rows = [pl.ds(h * hits + level_num * POINTS + p, 1) for p in range(POINTS)]
        for p in range(POINTS):
            mask_s[p * per_block:(p + 1) * per_block, :] = jnp.where(
                slot_row == point_s[b, 0, rows[p], :], 1.0, 0.0
            )
        cols = [
            hat(lane_row % side, point_s[b, 2, rows[p], :], corner_s[b, 2, rows[p], :],
                corner_s[b, 3, rows[p], :])
            for p in range(POINTS)
        ]
        rows_per_chunk = PACK // side

        def chunk(step, carry, rows=rows, cols=cols, side=side, span=span,
                  level_off=level_off, rows_per_chunk=rows_per_chunk):
            parts = []
            for p in range(POINTS):
                index = step * rows_per_chunk
                start = point_s[b, 1, rows[p], :]
                low = corner_s[b, 0, rows[p], :]
                high = corner_s[b, 1, rows[p], :]
                if rows_per_chunk > 1:
                    across = hat(index + lane_row // side, start, low, high)
                else:
                    across = jnp.where(
                        start == index, low, jnp.where(start == index - 1, high, 0.0)
                    )
                parts.append(cols[p] * across)
            for k in range(per_block):
                total = parts[0] * mask_s[k:k + 1, :]
                for p in range(1, POINTS):
                    total = total + parts[p] * mask_s[p * per_block + k:p * per_block + k + 1, :]
                where = pl.multiple_of(level_off + k * span + step * PACK, PACK)
                weight_s[slab, pl.ds(where, PACK), :] = total.astype(jnp.bfloat16)
            return carry

        chunks = span // PACK
        if chunks == 1:
            chunk(0, 0)
        else:
            lax.fori_loop(0, chunks, chunk, 0)
        level_off += span * per_block


def exchange_kernel(sides, spans, per_block, head_count, rows, cols, capacity, local_tiles, *refs):
    (table_ref, tiles_ref, query_ref, lw_ref, lb_ref, samples_ref, fetched_ref, weights_ref) = refs[:8]
    refs = refs[8:]
    held = refs[:cols - 1]
    (ids_v, stage, point_s, corner_s, mask_s, weight_s, id_send, id_recv, col_send, col_recv,
     row_send, row_recv, own_sem, ids_sem, weight_sem) = refs[cols - 1:]
    r = lax.axis_index("row")
    c = lax.axis_index("col")
    lanes_wide = tiles_ref.shape[1]
    barrier = pltpu.get_barrier_semaphore()
    for dc in range(1, cols):
        pl.semaphore_signal(barrier, inc=1, device_id={"col": lax.rem(c + dc, cols)}, device_id_type=MESH)
    for dr in range(1, rows):
        pl.semaphore_signal(barrier, inc=1, device_id={"row": lax.rem(r + dr, rows)}, device_id_type=MESH)
    pl.semaphore_wait(barrier, cols + rows - 2)

    id_copies = []
    for dr in range(1, rows):
        to = lax.rem(r + dr, rows)
        copy = pltpu.make_async_remote_copy(
            table_ref.at[to], ids_v.at[dr], id_send.at[dr], id_recv.at[dr],
            device_id={"row": to}, device_id_type=MESH,
        )
        copy.start()
        id_copies.append(copy)
    col_copies = []
    for dc in range(1, cols):
        copy = pltpu.make_async_remote_copy(
            tiles_ref, held[dc - 1], col_send.at[dc], col_recv.at[dc],
            device_id={"col": lax.rem(c + dc, cols)}, device_id_type=MESH,
        )
        copy.start()
        col_copies.append(copy)
    own_ids = pltpu.make_async_copy(table_ref.at[r], ids_v.at[0], ids_sem)
    own_ids.start()
    own_ids.wait()
    for copy in id_copies:
        copy.wait()

    def pick(dc):
        owner_col = lax.rem(c - dc + cols, cols)
        source = tiles_ref if dc == 0 else held[dc - 1]
        out_at = (r * cols + owner_col) * capacity
        copies = []
        for turn in range(rows):
            dr = (turn + 1) % rows
            for place in range(capacity):
                off = 0
                for level_num in range(LEVELS):
                    span = spans[level_num]
                    at = (owner_col * capacity + place) * LEVELS + level_num
                    asked = jnp.broadcast_to(ids_v[dr, pl.ds(at, 1), :], (PACK, lanes_wide))
                    shape = (span // PACK, PACK, lanes_wide)
                    total = None
                    for tile in range(local_tiles):
                        mask = jnp.where(asked == tile, 1.0, 0.0).astype(jnp.bfloat16)
                        first = local_tiles * off + tile * span
                        part = source[first:first + span, :].reshape(shape) * mask[None]
                        total = part if total is None else total + part
                    stage[dr, dc, place, off:off + span, :] = total.reshape(span, lanes_wide)
                    off += span
            target = fetched_ref.at[pl.ds(out_at, capacity)]
            if dr == 0:
                copy = pltpu.make_async_copy(stage.at[dr, dc], target, own_sem.at[dc])
            else:
                copy = pltpu.make_async_remote_copy(
                    stage.at[dr, dc], target, row_send.at[dr, dc], row_recv.at[dr, dc],
                    device_id={"row": lax.rem(r - dr + rows, rows)}, device_id_type=MESH,
                )
            copy.start()
            copies.append(copy)
        return copies

    copies = pick(0)

    def prepare_one(b, carry):
        prepare(head_count, b, query_ref, lw_ref, lb_ref, samples_ref, point_s, corner_s)
        return carry

    lax.fori_loop(0, local_tiles, prepare_one, 0)

    def store(step, slab):
        return pltpu.make_async_copy(
            weight_s.at[slab], weights_ref.at[step // head_count, step % head_count],
            weight_sem.at[slab],
        )

    def weigh_one(step, carry):
        slab = step % 2

        @pl.when(step >= 2)
        def _():
            store(step - 2, slab).wait()

        weigh(sides, spans, per_block, step // head_count, step % head_count, slab,
              point_s, corner_s, mask_s, weight_s)
        store(step, slab).start()
        return carry

    steps = local_tiles * head_count
    done = 0
    for dc in range(1, cols):
        until = steps * dc // (cols - 1)
        if until > done:
            lax.fori_loop(done, until, weigh_one, 0)
        done = until
        col_copies[dc - 1].wait()
        copies += pick(dc)
    for step in range(max(0, steps - 2), steps):
        store(step, step % 2).wait()
    for copy in copies:
        copy.wait()


def mix_kernel(spans, per_block, head_count, head_dim, pos_ref, fetched_ref, weight_ref, out_ref,
               values, values_t, mixed, sem):
    block = pl.program_id(0)
    h = pl.program_id(1)
    blocks = pl.num_programs(0)

    def fetch(which):
        off = 0
        src = 0
        for level_num in range(LEVELS):
            span = spans[level_num]
            for k in range(per_block):
                pltpu.make_async_copy(
                    fetched_ref.at[pos_ref[level_num, which * per_block + k], pl.ds(src, span), :],
                    values.at[which % 2, pl.ds(off, span), :],
                    sem.at[which % 2],
                ).start()
                off += span
            src += span

    @pl.when((h == 0) & (block == 0))
    def _():
        fetch(block)

    @pl.when(h == 0)
    def _():
        side = block % 2
        pltpu.make_async_copy(values.at[side], values.at[side], sem.at[side]).wait()
        values_t[...] = values[side].T.reshape(values_t.shape)

        @pl.when(block + 1 < blocks)
        def _():
            fetch(block + 1)

    mixed[h] = jnp.dot(values_t[h], weight_ref[0, 0], preferred_element_type=jnp.float32)

    @pl.when(h == head_count - 1)
    def _():
        whole = mixed[...].reshape(head_count * head_dim, mixed.shape[2])
        out_ref[...] = whole.T.astype(jnp.bfloat16)


def on_device(
    queries,
    level_zero,
    level_one,
    level_two,
    level_three,
    tile_lists,
    samples,
    logit_weight,
    logit_bias,
    output_weight,
    output_bias,
    norm_gain,
    norm_shift,
):
    level_blocks = (level_zero, level_one, level_two, level_three)
    row_count = lax.axis_size("row")
    col_count = lax.axis_size("col")
    peer_count = row_count * col_count
    tile_rows, tile_cols, level_count, per_block = tile_lists.shape
    local_tiles = tile_rows * tile_cols
    requests = local_tiles * per_block
    capacity = max(2, (requests + peer_count - 1) // peer_count)
    slots = peer_count * capacity
    grid_cols = tile_cols * col_count
    channels = level_zero.shape[2]
    width_all = queries.shape[2]
    head_count = samples.shape[2] // (LEVELS * POINTS)
    head_dim = channels // head_count
    tile_side = level_zero.shape[0] // tile_rows
    pixels = tile_side * tile_side
    sides = [level_blocks[level_num].shape[0] // tile_rows for level_num in range(level_count)]
    spans = [max(PACK, side * side) for side in sides]
    tile_span = sum(spans)
    depth = per_block * tile_span

    wanted = tile_lists.transpose(2, 0, 1, 3).reshape(level_count, requests)
    grid_row = wanted // grid_cols
    grid_col = wanted % grid_cols
    owner_dev = grid_row // tile_rows * col_count + grid_col // tile_cols
    local_index = grid_row % tile_rows * tile_cols + grid_col % tile_cols
    order = jnp.arange(requests, dtype=jnp.int32)
    earlier = (owner_dev[:, :, None] == owner_dev[:, None, :]) & (order[None, :] < order[:, None])
    positions = owner_dev * capacity + jnp.sum(earlier.astype(jnp.int32), axis=2)
    slot_order = jnp.arange(slots, dtype=jnp.int32)
    named = positions[:, None, :] == slot_order[None, :, None]
    slot_table = jnp.max(jnp.where(named, local_index[:, None, :], -1), axis=2)
    table = jnp.maximum(slot_table, 0).reshape(level_count, row_count, col_count * capacity)
    table = table.transpose(1, 2, 0).reshape(row_count, col_count * capacity * level_count, 1)
    table_rows = table.shape[1]
    table = jnp.broadcast_to(table, (row_count, table_rows, channels))

    tiles_local = []
    for level_num in range(level_count):
        tiles = to_blocks(level_blocks[level_num], tile_rows, tile_cols, sides[level_num])
        short = spans[level_num] - tiles.shape[1]
        if short > 0:
            tiles = jnp.pad(tiles, ((0, 0), (0, short), (0, 0)))
        tiles_local.append(tiles.reshape(local_tiles * spans[level_num], channels))
    tiles_local = jnp.concatenate(tiles_local, axis=0)

    queries_blocked = to_blocks(queries, tile_rows, tile_cols, tile_side)
    samples_t = to_blocks(samples, tile_rows, tile_cols, tile_side).transpose(0, 2, 1)
    lanes = head_count * LEVELS * POINTS
    vmem = pl.BlockSpec(memory_space=pltpu.VMEM)
    whole = pl.BlockSpec(memory_space=pl.ANY)
    dma = pltpu.SemaphoreType.DMA
    fetched, weights = pl.pallas_call(
        functools.partial(exchange_kernel, sides, spans, per_block, head_count, row_count,
                          col_count, capacity, local_tiles),
        out_shape=(
            jax.ShapeDtypeStruct((slots, tile_span, channels), jnp.bfloat16),
            jax.ShapeDtypeStruct((local_tiles, head_count, depth, pixels), jnp.bfloat16),
        ),
        in_specs=[vmem] * 6,
        out_specs=(whole, whole),
        scratch_shapes=[
            pltpu.VMEM((local_tiles * tile_span, channels), jnp.bfloat16)
            for _ in range(col_count - 1)
        ] + [
            pltpu.VMEM((row_count, table_rows, channels), jnp.int32),
            pltpu.VMEM((row_count, col_count, capacity, tile_span, channels), jnp.bfloat16),
            pltpu.VMEM((local_tiles, 3, lanes, pixels), jnp.int32),
            pltpu.VMEM((local_tiles, 4, lanes, pixels), jnp.float32),
            pltpu.VMEM((POINTS * per_block, pixels), jnp.float32),
            pltpu.VMEM((2, depth, pixels), jnp.bfloat16),
            dma((row_count,)), dma((row_count,)), dma((col_count,)), dma((col_count,)),
            dma((row_count, col_count)), dma((row_count, col_count)), dma((col_count,)),
            dma, dma((2,)),
        ],
        compiler_params=pltpu.CompilerParams(
            collective_id=0, has_side_effects=True, vmem_limit_bytes=60 * 1024 * 1024
        ),
        cost_estimate=pl.CostEstimate(
            flops=8 * local_tiles * head_count * depth * pixels * POINTS,
            bytes_accessed=2 * local_tiles * head_count * depth * pixels, transcendentals=0,
        ),
        name="exchange",
    )(table, tiles_local, queries_blocked, logit_weight.T, logit_bias[:, None], samples_t)

    attn_out = pl.pallas_call(
        functools.partial(mix_kernel, spans, per_block, head_count, head_dim),
        grid_spec=pltpu.PrefetchScalarGridSpec(
            num_scalar_prefetch=1,
            grid=(local_tiles, head_count),
            in_specs=[
                pl.BlockSpec(memory_space=pl.ANY),
                pl.BlockSpec((1, 1, depth, pixels), lambda b, h, pos: (b, h, 0, 0)),
            ],
            out_specs=pl.BlockSpec((pixels, channels), lambda b, h, pos: (b, 0)),
            scratch_shapes=[
                pltpu.VMEM((2, depth, channels), jnp.bfloat16),
                pltpu.VMEM((head_count, head_dim, depth), jnp.bfloat16),
                pltpu.VMEM((head_count, head_dim, pixels), jnp.float32),
                pltpu.SemaphoreType.DMA((2,)),
            ],
        ),
        out_shape=jax.ShapeDtypeStruct((local_tiles * pixels, channels), jnp.bfloat16),
        compiler_params=pltpu.CompilerParams(
            dimension_semantics=("arbitrary", "arbitrary"), vmem_limit_bytes=60 * 1024 * 1024
        ),
        cost_estimate=pl.CostEstimate(
            flops=2 * local_tiles * depth * pixels * channels,
            bytes_accessed=2 * local_tiles * head_count * depth * pixels, transcendentals=0,
        ),
        name="mix",
    )(positions, fetched, weights)

    head_index = lax.axis_index("head")
    full_attn = lax.all_gather(attn_out, "head", axis=1, tiled=True)
    pre_norm = (
        queries_blocked.reshape(local_tiles * pixels, width_all).astype(jnp.float32)
        + jnp.dot(full_attn, output_weight, preferred_element_type=jnp.float32)
        + output_bias
    )
    row_mean = jnp.mean(pre_norm, axis=1, keepdims=True)
    centered = pre_norm - row_mean
    variance = jnp.mean(centered * centered, axis=1, keepdims=True)
    own_part = lax.dynamic_slice_in_dim(centered, head_index * channels, channels, 1)
    normalized = own_part * lax.rsqrt(variance + 1e-05)
    updated = (normalized * norm_gain + norm_shift).astype(jnp.bfloat16)
    updated = updated.reshape(tile_rows, tile_cols, tile_side, tile_side, channels).transpose(
        0, 2, 1, 3, 4
    )
    return updated.reshape(tile_rows * tile_side, tile_cols * tile_side, channels)


def solution(mesh):
    in_specs = (
        P("row", "col", None),
        P("row", "col", "head"),
        P("row", "col", "head"),
        P("row", "col", "head"),
        P("row", "col", "head"),
        P("row", "col", None, None),
        P("row", "col", "head"),
        P(None, "head"),
        P("head"),
        P(),
        P(),
        P("head"),
        P("head"),
    )
    out_specs = P("row", "col", "head")
    return jax.shard_map(
        on_device, mesh=mesh, in_specs=in_specs, out_specs=out_specs, check_vma=False
    )
```

```python
import functools

import jax
import jax.numpy as jnp
from jax import lax
from jax.experimental import pallas as pl
from jax.experimental.pallas import tpu as pltpu
from jax.sharding import PartitionSpec as P

LEVELS = 4
POINTS = 4
PACK = 16
MESH = pl.DeviceIdType.MESH


def to_blocks(source, tile_rows, tile_cols, tile_side):
    channels = source.shape[2]
    shaped = source.reshape(tile_rows, tile_side, tile_cols, tile_side, channels)
    return shaped.transpose(0, 2, 1, 3, 4).reshape(
        tile_rows * tile_cols, tile_side * tile_side, channels
    )


def hat(index, start, low, high):
    return jnp.where(index == start, low, jnp.where(index == start + 1, high, 0.0))


def prepare(head_count, b, query_ref, lw_ref, lb_ref, samples_ref, point_s, corner_s):
    queries_here = query_ref.shape[1]
    hits = LEVELS * POINTS
    logits = lax.dot_general(
        lw_ref[...], query_ref[b], (((1,), (1,)), ((), ())), preferred_element_type=jnp.float32
    ) + lb_ref[...]
    logits = logits.reshape(head_count, hits, queries_here)
    shifted = jnp.exp(logits - jnp.max(logits, axis=1, keepdims=True))
    attend = shifted / jnp.sum(shifted, axis=1, keepdims=True)
    attend = attend.reshape(head_count * hits, queries_here)
    packed = samples_ref[b].T
    pos_row = (packed >> 12) & 4095
    pos_col = packed & 4095
    frac_row = (pos_row & 255).astype(jnp.float32) * (1.0 / 256.0)
    frac_col = (pos_col & 255).astype(jnp.float32) * (1.0 / 256.0)
    point_s[b, 0] = packed >> 24
    point_s[b, 1] = pos_row >> 8
    point_s[b, 2] = pos_col >> 8
    corner_s[b, 0] = attend * (1.0 - frac_row)
    corner_s[b, 1] = attend * frac_row
    corner_s[b, 2] = 1.0 - frac_col
    corner_s[b, 3] = frac_col


def weigh(sides, spans, per_block, b, h, slab, point_s, corner_s, mask_s, weight_s):
    hits = LEVELS * POINTS
    queries_here = weight_s.shape[2]
    lane_row = lax.broadcasted_iota(jnp.int32, (PACK, queries_here), 0)
    slot_row = lax.broadcasted_iota(jnp.int32, (per_block, queries_here), 0)
    level_off = 0
    for level_num in range(LEVELS):
        side = sides[level_num]
        span = spans[level_num]
        rows = [pl.ds(h * hits + level_num * POINTS + p, 1) for p in range(POINTS)]
        for p in range(POINTS):
            mask_s[p * per_block:(p + 1) * per_block, :] = jnp.where(
                slot_row == point_s[b, 0, rows[p], :], 1.0, 0.0
            )
        cols = [
            hat(lane_row % side, point_s[b, 2, rows[p], :], corner_s[b, 2, rows[p], :],
                corner_s[b, 3, rows[p], :])
            for p in range(POINTS)
        ]
        rows_per_chunk = PACK // side

        def chunk(step, carry, rows=rows, cols=cols, side=side, span=span,
                  level_off=level_off, rows_per_chunk=rows_per_chunk):
            parts = []
            for p in range(POINTS):
                index = step * rows_per_chunk
                start = point_s[b, 1, rows[p], :]
                low = corner_s[b, 0, rows[p], :]
                high = corner_s[b, 1, rows[p], :]
                if rows_per_chunk > 1:
                    across = hat(index + lane_row // side, start, low, high)
                else:
                    across = jnp.where(
                        start == index, low, jnp.where(start == index - 1, high, 0.0)
                    )
                parts.append(cols[p] * across)
            for k in range(per_block):
                total = parts[0] * mask_s[k:k + 1, :]
                for p in range(1, POINTS):
                    total = total + parts[p] * mask_s[p * per_block + k:p * per_block + k + 1, :]
                where = pl.multiple_of(level_off + k * span + step * PACK, PACK)
                weight_s[slab, pl.ds(where, PACK), :] = total.astype(jnp.bfloat16)
            return carry

        chunks = span // PACK
        if chunks == 1:
            chunk(0, 0)
        else:
            lax.fori_loop(0, chunks, chunk, 0)
        level_off += span * per_block


def exchange_kernel(sides, spans, per_block, head_count, rows, cols, capacity, local_tiles, *refs):
    (table_ref, tiles_ref, query_ref, lw_ref, lb_ref, samples_ref, fetched_ref, weights_ref) = refs[:8]
    refs = refs[8:]
    held = refs[:cols - 1]
    (ids_v, stage, point_s, corner_s, mask_s, weight_s, id_send, id_recv, col_send, col_recv,
     row_send, row_recv, own_sem, ids_sem, weight_sem) = refs[cols - 1:]
    r = lax.axis_index("row")
    c = lax.axis_index("col")
    lanes_wide = tiles_ref.shape[1]
    barrier = pltpu.get_barrier_semaphore()
    for dc in range(1, cols):
        pl.semaphore_signal(barrier, inc=1, device_id={"col": lax.rem(c + dc, cols)}, device_id_type=MESH)
    for dr in range(1, rows):
        pl.semaphore_signal(barrier, inc=1, device_id={"row": lax.rem(r + dr, rows)}, device_id_type=MESH)
    pl.semaphore_wait(barrier, cols + rows - 2)

    id_copies = []
    for dr in range(1, rows):
        to = lax.rem(r + dr, rows)
        copy = pltpu.make_async_remote_copy(
            table_ref.at[to], ids_v.at[dr], id_send.at[dr], id_recv.at[dr],
            device_id={"row": to}, device_id_type=MESH,
        )
        copy.start()
        id_copies.append(copy)
    col_copies = []
    for dc in range(1, cols):
        copy = pltpu.make_async_remote_copy(
            tiles_ref, held[dc - 1], col_send.at[dc], col_recv.at[dc],
            device_id={"col": lax.rem(c + dc, cols)}, device_id_type=MESH,
        )
        copy.start()
        col_copies.append(copy)
    own_ids = pltpu.make_async_copy(table_ref.at[r], ids_v.at[0], ids_sem)
    own_ids.start()
    own_ids.wait()
    for copy in id_copies:
        copy.wait()

    def pick(dc):
        owner_col = lax.rem(c - dc + cols, cols)
        source = tiles_ref if dc == 0 else held[dc - 1]
        out_at = (r * cols + owner_col) * capacity
        copies = []
        for turn in range(rows):
            dr = (turn + 1) % rows
            for place in range(capacity):
                off = 0
                for level_num in range(LEVELS):
                    span = spans[level_num]
                    at = (owner_col * capacity + place) * LEVELS + level_num
                    asked = jnp.broadcast_to(ids_v[dr, pl.ds(at, 1), :], (PACK, lanes_wide))
                    shape = (span // PACK, PACK, lanes_wide)
                    total = None
                    for tile in range(local_tiles):
                        mask = jnp.where(asked == tile, 1.0, 0.0).astype(jnp.bfloat16)
                        first = local_tiles * off + tile * span
                        part = source[first:first + span, :].reshape(shape) * mask[None]
                        total = part if total is None else total + part
                    stage[dr, dc, place, off:off + span, :] = total.reshape(span, lanes_wide)
                    off += span
            target = fetched_ref.at[pl.ds(out_at, capacity)]
            if dr == 0:
                copy = pltpu.make_async_copy(stage.at[dr, dc], target, own_sem.at[dc])
            else:
                copy = pltpu.make_async_remote_copy(
                    stage.at[dr, dc], target, row_send.at[dr, dc], row_recv.at[dr, dc],
                    device_id={"row": lax.rem(r - dr + rows, rows)}, device_id_type=MESH,
                )
            copy.start()
            copies.append(copy)
        return copies

    copies = pick(0)

    def prepare_one(b, carry):
        prepare(head_count, b, query_ref, lw_ref, lb_ref, samples_ref, point_s, corner_s)
        return carry

    lax.fori_loop(0, local_tiles, prepare_one, 0)

    def store(step, slab):
        return pltpu.make_async_copy(
            weight_s.at[slab], weights_ref.at[step // head_count, step % head_count],
            weight_sem.at[slab],
        )

    def weigh_one(step, carry):
        slab = step % 2

        @pl.when(step >= 2)
        def _():
            store(step - 2, slab).wait()

        weigh(sides, spans, per_block, step // head_count, step % head_count, slab,
              point_s, corner_s, mask_s, weight_s)
        store(step, slab).start()
        return carry

    steps = local_tiles * head_count
    done = 0
    for dc in range(1, cols):
        until = steps * dc // (cols - 1)
        if until > done:
            lax.fori_loop(done, until, weigh_one, 0)
        done = until
        col_copies[dc - 1].wait()
        copies += pick(dc)
    for step in range(max(0, steps - 2), steps):
        store(step, step % 2).wait()
    for copy in copies:
        copy.wait()


def mix_kernel(spans, per_block, head_count, head_dim, pos_ref, fetched_ref, upper_ref, lower_ref,
               out_ref,
               values, values_t, mixed, sem):
    block = pl.program_id(0)
    h = pl.program_id(1)
    blocks = pl.num_programs(0)

    def fetch(which):
        off = 0
        src = 0
        for level_num in range(LEVELS):
            span = spans[level_num]
            for k in range(per_block):
                pltpu.make_async_copy(
                    fetched_ref.at[pos_ref[level_num, which * per_block + k], pl.ds(src, span), :],
                    values.at[which % 2, pl.ds(off, span), :],
                    sem.at[which % 2],
                ).start()
                off += span
            src += span

    @pl.when((h == 0) & (block == 0))
    def _():
        fetch(block)

    @pl.when(h == 0)
    def _():
        side = block % 2
        pltpu.make_async_copy(values.at[side], values.at[side], sem.at[side]).wait()
        values_t[...] = values[side].T.reshape(values_t.shape)

        @pl.when(block + 1 < blocks)
        def _():
            fetch(block + 1)

    half = upper_ref.shape[2]
    mixed[h] = jnp.dot(
        values_t[h, :, :half], upper_ref[0, 0], preferred_element_type=jnp.float32
    ) + jnp.dot(values_t[h, :, half:], lower_ref[0, 0], preferred_element_type=jnp.float32)

    @pl.when(h == head_count - 1)
    def _():
        whole = mixed[...].reshape(head_count * head_dim, mixed.shape[2])
        out_ref[...] = whole.T.astype(jnp.bfloat16)


def on_device(
    queries,
    level_zero,
    level_one,
    level_two,
    level_three,
    tile_lists,
    samples,
    logit_weight,
    logit_bias,
    output_weight,
    output_bias,
    norm_gain,
    norm_shift,
):
    level_blocks = (level_zero, level_one, level_two, level_three)
    row_count = lax.axis_size("row")
    col_count = lax.axis_size("col")
    peer_count = row_count * col_count
    tile_rows, tile_cols, level_count, per_block = tile_lists.shape
    local_tiles = tile_rows * tile_cols
    requests = local_tiles * per_block
    capacity = max(2, (requests + peer_count - 1) // peer_count)
    slots = peer_count * capacity
    grid_cols = tile_cols * col_count
    channels = level_zero.shape[2]
    width_all = queries.shape[2]
    head_count = samples.shape[2] // (LEVELS * POINTS)
    head_dim = channels // head_count
    tile_side = level_zero.shape[0] // tile_rows
    pixels = tile_side * tile_side
    sides = [level_blocks[level_num].shape[0] // tile_rows for level_num in range(level_count)]
    spans = [max(PACK, side * side) for side in sides]
    tile_span = sum(spans)
    depth = per_block * tile_span

    wanted = tile_lists.transpose(2, 0, 1, 3).reshape(level_count, requests)
    grid_row = wanted // grid_cols
    grid_col = wanted % grid_cols
    owner_dev = grid_row // tile_rows * col_count + grid_col // tile_cols
    local_index = grid_row % tile_rows * tile_cols + grid_col % tile_cols
    order = jnp.arange(requests, dtype=jnp.int32)
    earlier = (owner_dev[:, :, None] == owner_dev[:, None, :]) & (order[None, :] < order[:, None])
    positions = owner_dev * capacity + jnp.sum(earlier.astype(jnp.int32), axis=2)
    slot_order = jnp.arange(slots, dtype=jnp.int32)
    named = positions[:, None, :] == slot_order[None, :, None]
    slot_table = jnp.max(jnp.where(named, local_index[:, None, :], -1), axis=2)
    table = jnp.maximum(slot_table, 0).reshape(level_count, row_count, col_count * capacity)
    table = table.transpose(1, 2, 0).reshape(row_count, col_count * capacity * level_count, 1)
    table_rows = table.shape[1]
    table = jnp.broadcast_to(table, (row_count, table_rows, channels))

    tiles_local = []
    for level_num in range(level_count):
        tiles = to_blocks(level_blocks[level_num], tile_rows, tile_cols, sides[level_num])
        short = spans[level_num] - tiles.shape[1]
        if short > 0:
            tiles = jnp.pad(tiles, ((0, 0), (0, short), (0, 0)))
        tiles_local.append(tiles.reshape(local_tiles * spans[level_num], channels))
    tiles_local = jnp.concatenate(tiles_local, axis=0)

    queries_blocked = to_blocks(queries, tile_rows, tile_cols, tile_side)
    samples_blocked = to_blocks(samples, tile_rows, tile_cols, tile_side)
    lanes = head_count * LEVELS * POINTS
    vmem = pl.BlockSpec(memory_space=pltpu.VMEM)
    whole = pl.BlockSpec(memory_space=pl.ANY)
    dma = pltpu.SemaphoreType.DMA
    fetched, weights = pl.pallas_call(
        functools.partial(exchange_kernel, sides, spans, per_block, head_count, row_count,
                          col_count, capacity, local_tiles),
        out_shape=(
            jax.ShapeDtypeStruct((slots, tile_span, channels), jnp.bfloat16),
            jax.ShapeDtypeStruct((local_tiles, head_count, depth, pixels), jnp.bfloat16),
        ),
        in_specs=[vmem] * 6,
        out_specs=(whole, whole),
        scratch_shapes=[
            pltpu.VMEM((local_tiles * tile_span, channels), jnp.bfloat16)
            for _ in range(col_count - 1)
        ] + [
            pltpu.VMEM((row_count, table_rows, channels), jnp.int32),
            pltpu.VMEM((row_count, col_count, capacity, tile_span, channels), jnp.bfloat16),
            pltpu.VMEM((local_tiles, 3, lanes, pixels), jnp.int32),
            pltpu.VMEM((local_tiles, 4, lanes, pixels), jnp.float32),
            pltpu.VMEM((POINTS * per_block, pixels), jnp.float32),
            pltpu.VMEM((2, depth, pixels), jnp.bfloat16),
            dma((row_count,)), dma((row_count,)), dma((col_count,)), dma((col_count,)),
            dma((row_count, col_count)), dma((row_count, col_count)), dma((col_count,)),
            dma, dma((2,)),
        ],
        compiler_params=pltpu.CompilerParams(
            collective_id=0, has_side_effects=True, vmem_limit_bytes=60 * 1024 * 1024
        ),
        cost_estimate=pl.CostEstimate(
            flops=8 * local_tiles * head_count * depth * pixels * POINTS,
            bytes_accessed=2 * local_tiles * head_count * depth * pixels, transcendentals=0,
        ),
        name="exchange",
    )(table, tiles_local, queries_blocked, logit_weight.T, logit_bias[:, None], samples_blocked)

    attn_out = pl.pallas_call(
        functools.partial(mix_kernel, spans, per_block, head_count, head_dim),
        grid_spec=pltpu.PrefetchScalarGridSpec(
            num_scalar_prefetch=1,
            grid=(local_tiles, head_count),
            in_specs=[
                pl.BlockSpec(memory_space=pl.ANY),
                pl.BlockSpec((1, 1, depth // 2, pixels), lambda b, h, pos: (b, h, 0, 0)),
                pl.BlockSpec((1, 1, depth // 2, pixels), lambda b, h, pos: (b, h, 1, 0)),
            ],
            out_specs=pl.BlockSpec((pixels, channels), lambda b, h, pos: (b, 0)),
            scratch_shapes=[
                pltpu.VMEM((2, depth, channels), jnp.bfloat16),
                pltpu.VMEM((head_count, head_dim, depth), jnp.bfloat16),
                pltpu.VMEM((head_count, head_dim, pixels), jnp.float32),
                pltpu.SemaphoreType.DMA((2,)),
            ],
        ),
        out_shape=jax.ShapeDtypeStruct((local_tiles * pixels, channels), jnp.bfloat16),
        compiler_params=pltpu.CompilerParams(
            dimension_semantics=("arbitrary", "arbitrary"), vmem_limit_bytes=60 * 1024 * 1024
        ),
        cost_estimate=pl.CostEstimate(
            flops=2 * local_tiles * depth * pixels * channels,
            bytes_accessed=2 * local_tiles * head_count * depth * pixels, transcendentals=0,
        ),
        name="mix",
    )(positions, fetched, weights, weights)

    head_index = lax.axis_index("head")
    full_attn = lax.all_gather(attn_out, "head", axis=1, tiled=True)
    pre_norm = (
        queries_blocked.reshape(local_tiles * pixels, width_all).astype(jnp.float32)
        + jnp.dot(full_attn, output_weight, preferred_element_type=jnp.float32)
        + output_bias
    )
    row_mean = jnp.mean(pre_norm, axis=1, keepdims=True)
    centered = pre_norm - row_mean
    variance = jnp.mean(centered * centered, axis=1, keepdims=True)
    own_part = lax.dynamic_slice_in_dim(centered, head_index * channels, channels, 1)
    normalized = own_part * lax.rsqrt(variance + 1e-05)
    updated = (normalized * norm_gain + norm_shift).astype(jnp.bfloat16)
    updated = updated.reshape(tile_rows, tile_cols, tile_side, tile_side, channels).transpose(
        0, 2, 1, 3, 4
    )
    return updated.reshape(tile_rows * tile_side, tile_cols * tile_side, channels)


def solution(mesh):
    in_specs = (
        P("row", "col", None),
        P("row", "col", "head"),
        P("row", "col", "head"),
        P("row", "col", "head"),
        P("row", "col", "head"),
        P("row", "col", None, None),
        P("row", "col", "head"),
        P(None, "head"),
        P("head"),
        P(),
        P(),
        P("head"),
        P("head"),
    )
    out_specs = P("row", "col", "head")
    return jax.shard_map(
        on_device, mesh=mesh, in_specs=in_specs, out_specs=out_specs, check_vma=False
    )
```
